32 devices in a mesh: pool: 4 (over y, core), ga: 8 (over z, x).
Axes of the slice: x: 2, y: 2, z: 4, core: 2. Of those that a mesh axis runs over, the one named last changes fastest.
Arguments:
- coefficients: bfloat16 [4, 256, 2, 256, 128], P('pool', 'ga'), may hold values from -6 to 6
- stick_count: int32 [4, 8], P('pool', 'ga'), may hold values from 28 to 32, as said below
- dest_device: int32 [4, 256], P('pool', 'ga'), may hold values from -1 to 7, as said below
- dest_slot: int32 [4, 256], P('pool', 'ga'), may hold values from -1 to 31, as said below
- source_stick: int32 [4, 256], P('pool', 'ga'), may hold values from -1 to 255, as said below
Outputs:
- margins: float32 [4, 2, 256, 256], P('pool', None, 'ga')
The draws below stay inside these ranges and needn't reach their ends.
Inputs may be any that keep to these rules, and one draw needn't show every extreme that they name: Every k-point has a device whose 32 slots are all live; a device's live sticks are its first stick_count slots. `dest_device`: -1 exactly for sticks that land nowhere (among them all sticks that are not live); no device sends more than 8 of its sticks to one device, and some pair of devices reaches 8 for every k-point. `dest_slot`: -1 where dest_device is -1; the slots named are live slots of the layout of k-point q-1, no slot named twice. `source_stick`: the exact inverse of dest_device and dest_slot: a slot names a stick exactly when that stick names the slot, else -1.
All inputs are finite; a program needn't handle non-finite values.
Results may differ from the reference program's by a relative error of at most 0.0003.
Values may be sent and summed in bfloat16 or wider, within the bound.
No kernel may reach another device: no remote copies, remote signals or barrier semaphores. Data moves between devices by JAX's collectives and lax.ppermute only.
A program may use at most 64 MiB of HBM per device.

```python
import jax
import jax.numpy as jnp
from jax import lax

NB = 256
PW = 128
SLOTS = 32
KPTS = 4
STICKS = 256
CAP = 8
N_GA = 8


def stick_maps(key):
    base_key = jax.random.fold_in(key, 7101)
    subkeys = jax.random.split(base_key, 6)
    lowest = SLOTS - max(1, SLOTS // 8)
    counts = jax.random.randint(subkeys[0], (KPTS, N_GA), lowest, SLOTS + 1)
    shifts = jax.random.randint(subkeys[1], (KPTS,), 0, N_GA)
    offsets = jax.vmap(lambda sub: jax.random.permutation(sub, N_GA))(jax.random.split(subkeys[2], KPTS))
    dest_order = jax.vmap(lambda sub: jax.random.permutation(sub, SLOTS))(jax.random.split(subkeys[3], KPTS * N_GA)).reshape(KPTS, N_GA, SLOTS)
    source_order = jax.vmap(lambda sub: jax.random.permutation(sub, SLOTS))(jax.random.split(subkeys[4], KPTS * N_GA)).reshape(KPTS, N_GA, SLOTS)
    full_dest = jax.random.randint(subkeys[5], (KPTS,), 0, N_GA)
    kpoint_list = jnp.arange(KPTS)
    counts = counts.at[(kpoint_list - 1) % KPTS, full_dest].set(SLOTS)
    full_source = (full_dest + shifts + offsets[:, 0]) % N_GA
    counts = counts.at[kpoint_list, full_source].set(SLOTS)
    shape = (KPTS, N_GA, SLOTS)
    device_grid = jnp.broadcast_to(jnp.arange(N_GA)[None, :, None], shape)
    kpoint_grid = jnp.broadcast_to(kpoint_list[:, None, None], shape)
    block_of = jnp.arange(SLOTS) // CAP
    chosen = offsets[:, block_of][:, None, :]
    source_dev = (device_grid + shifts[:, None, None] + chosen) % N_GA
    source_slot = jnp.take_along_axis(source_order, source_dev, axis=1)
    prev_counts = jnp.roll(counts, 1, axis=0)
    dest_live = dest_order < prev_counts[:, :, None]
    source_counts = jnp.take_along_axis(counts, source_dev.reshape(KPTS, N_GA * SLOTS), axis=1).reshape(shape)
    source_live = source_slot < source_counts
    valid = dest_live & source_live
    empty = jnp.full(shape, -1, jnp.int32)
    source_stick = empty.at[kpoint_grid, device_grid, dest_order].set(jnp.where(valid, source_dev * SLOTS + source_slot, -1).astype(jnp.int32))
    dest_device = empty.at[kpoint_grid, source_dev, source_slot].set(jnp.where(valid, device_grid, -1).astype(jnp.int32))
    dest_slot = empty.at[kpoint_grid, source_dev, source_slot].set(jnp.where(valid, dest_order, -1).astype(jnp.int32))
    flat_shape = (KPTS, N_GA * SLOTS)
    return (counts.astype(jnp.int32), dest_device.reshape(flat_shape), dest_slot.reshape(flat_shape), source_stick.reshape(flat_shape))


def draw_stick_count(key, part):
    return stick_maps(key)[0]


def draw_dest_device(key, part):
    return stick_maps(key)[1]


def draw_dest_slot(key, part):
    return stick_maps(key)[2]


def draw_source_stick(key, part):
    return stick_maps(key)[3]


def block_scale(own_key, dims, cuts, low, top_value):
    def one(position, shards_of):
        heights = jax.random.uniform(jax.random.fold_in(jax.random.fold_in(own_key, 6), position), (shards_of,), jnp.float32, low / len(cuts), top_value / len(cuts))
        return jnp.repeat(jnp.exp(heights), dims[position] // shards_of).reshape((-1,) + (1,) * (len(dims) - position - 1))

    gain = one(*cuts[0])
    for cut in cuts[1:]:
        gain = gain * one(*cut)
    return gain


def noise(own_key, extent, width, bound, pieces=(), kind=jnp.bfloat16):
    array = jax.random.normal(own_key, extent, jnp.float32) * width
    if len(pieces) > 0:
        array = block_scale(own_key, extent, pieces, -0.22, 0.18) * array
    return jnp.clip(array, min=-bound, max=bound).astype(kind)


def setup_inputs(seed: int = 0) -> dict:
    streams_of = jax.random.split(jax.random.key(seed), 6)
    coefficients = noise(streams_of[0], (KPTS, STICKS, 2, NB, PW), 1.0, 6.0, ((0, 4), (1, 8)))
    stick_count = draw_stick_count(jax.random.fold_in(streams_of[5], 71), 0)
    dest_device = draw_dest_device(jax.random.fold_in(streams_of[5], 71), 0)
    dest_slot = draw_dest_slot(jax.random.fold_in(streams_of[5], 71), 0)
    source_stick = draw_source_stick(jax.random.fold_in(streams_of[5], 71), 0)
    return {"coefficients": coefficients, "stick_count": stick_count, "dest_device": dest_device, "dest_slot": dest_slot, "source_stick": source_stick}


def reference(coefficients, stick_count, dest_device, dest_slot, source_stick):
    norm_scale = jnp.float32((2 * STICKS * PW) ** -0.5)
    slot_index = (jnp.arange(STICKS) % SLOTS).astype(jnp.int32)
    owner_device = (jnp.arange(STICKS) // SLOTS).astype(jnp.int32)
    results = []
    for kpoint in range(KPTS):
        neighbour = (kpoint + 1) % KPTS
        live_mask = slot_index < stick_count[kpoint][owner_device]
        bra_rows = jnp.where(live_mask[:, None, None, None], coefficients[kpoint], 0).astype(jnp.float32)
        anchor = source_stick[neighbour]
        safe_index = jnp.clip(anchor, 0, STICKS - 1).astype(jnp.int32)
        agreeing = (anchor >= 0) & (dest_device[neighbour][safe_index] == owner_device) & (dest_slot[neighbour][safe_index] == slot_index)
        ket_rows = jnp.where(agreeing[:, None, None, None], coefficients[neighbour][safe_index], 0).astype(jnp.float32)
        swapped = jnp.stack([ket_rows[:, 1], -ket_rows[:, 0]], axis=1)
        real_part = jnp.einsum('scmg,scng->mn', bra_rows, ket_rows, precision=lax.Precision.HIGHEST)
        imag_part = jnp.einsum('scmg,scng->mn', bra_rows, swapped, precision=lax.Precision.HIGHEST)
        results.append(jnp.stack([real_part, imag_part]) * norm_scale)
    return jnp.stack(results)
```

```python
import jax
import jax.numpy as jnp
from jax import lax
from jax.experimental import pallas as pl
from jax.experimental.pallas import tpu as pltpu
from jax.sharding import PartitionSpec as P


def swapped_with(value, distance):
    count = lax.axis_size("ga")
    return lax.ppermute(value, "ga", [(i, i ^ distance) for i in range(count)])


def to_previous_pool(value):
    count = lax.axis_size("pool")
    return lax.ppermute(value, "pool", [(i, (i - 1) % count) for i in range(count)])


def pack(x, groups, me):
    slots, _, bands, waves = x.shape
    part = waves // groups
    if part % 16:
        cut = x.reshape(slots, 2, bands, groups, part).transpose(3, 1, 0, 4, 2)
        return [lax.dynamic_index_in_dim(cut, me ^ d, 0, False) for d in range(groups)]
    step = 8 if slots % 8 == 0 else 1

    def body(select_ref, x_ref, *outs):
        for s in range(step):
            for c in range(2):
                turned = lax.dot_general(
                    select_ref[...],
                    x_ref[s, c],
                    (((1,), (1,)), ((), ())),
                    preferred_element_type=jnp.float32,
                ).astype(jnp.bfloat16)
                for d in range(groups):
                    outs[d][c, s] = turned[d * part : (d + 1) * part]

    row = jnp.arange(waves, dtype=jnp.int32)
    source = ((row // part) ^ me) * part + row % part
    select = (source[:, None] == row[None, :]).astype(jnp.bfloat16)
    return pl.pallas_call(
        body,
        grid=(slots // step,),
        in_specs=[
            pl.BlockSpec((waves, waves), lambda i: (0, 0)),
            pl.BlockSpec((step, 2, bands, waves), lambda i: (i, 0, 0, 0)),
        ],
        out_specs=[pl.BlockSpec((2, step, part, bands), lambda i: (0, i, 0, 0))] * groups,
        out_shape=[jax.ShapeDtypeStruct((2, slots, part, bands), jnp.bfloat16)] * groups,
    )(select, x)


def pair_list(stick_count, dest_device, dest_slot, source_stick, groups, slots, me):
    mine = jnp.concatenate([stick_count, dest_device, dest_slot, source_stick], axis=1)
    every = lax.all_gather(mine[0], ("pool", "ga"))
    pools = lax.axis_size("pool")
    every = every.reshape(pools, groups, 1 + 3 * slots)
    pool = lax.axis_index("pool")
    counts = lax.dynamic_index_in_dim(every, pool, 0, False)[:, 0]
    maps = lax.dynamic_index_in_dim(every, (pool + 1) % pools, 0, False)[:, 1:]
    maps = maps.reshape(groups, 3, slots).transpose(1, 0, 2).reshape(3, groups * slots)
    device, slot, anchor = maps[0], maps[1], maps[2]
    number = jnp.arange(groups * slots, dtype=jnp.int32)
    here = ((number // slots) ^ me) * slots + number % slots
    lands = jnp.where(device >= 0, device * slots + slot, -1)
    at_slot = here[:, None] == number[None, :]
    wanted = jnp.sum(jnp.where(at_slot, anchor[None, :], 0), axis=1)
    owner = jnp.arange(groups, dtype=jnp.int32)
    live = jnp.sum(jnp.where((here // slots)[:, None] == owner[None, :], counts[None, :], 0), axis=1)
    agreeing = (wanted[:, None] == number[None, :]) & (lands[None, :] == here[:, None])
    agreeing &= (here % slots < live)[:, None]
    return jnp.max(jnp.where(agreeing, here[None, :], -1), axis=1)


def multiply(bras, kets, pairs, me, groups, scale):
    _, slots, part, bands = bras[0].shape
    rows = bands // groups
    if part % 16:
        bra = jnp.concatenate(bras, axis=1)
        ket = jnp.concatenate(kets, axis=1)[:, jnp.maximum(pairs, 0)]
        ket = jnp.where((pairs >= 0)[None, :, None, None], ket, jnp.zeros_like(ket))

        def dot(a, b):
            return jnp.einsum("trm,trn->mn", bra[a], ket[b], preferred_element_type=jnp.float32)

        total = jnp.stack([dot(0, 0) + dot(1, 1), dot(0, 1) - dot(1, 0)]) * scale
        total = total.reshape(2, groups, rows, bands).transpose(1, 0, 2, 3)
        order = jnp.arange(groups, dtype=jnp.int32) ^ me
        total = total[order]
        return total[1::2], total[0::2]
    depth = slots * part

    def body(me_ref, pairs_ref, *refs):
        bra_refs, ket_refs = refs[:groups], refs[groups : 2 * groups]
        give_ref, keep_ref, bra_all, ket_all, chosen, total, bra_sem, ket_sem = refs[2 * groups :]
        ket_copies = [
            pltpu.make_async_copy(ket_refs[d], ket_all.at[:, pl.ds(d * slots, slots)], ket_sem.at[d])
            for d in range(groups)
        ]
        bra_copies = [
            pltpu.make_async_copy(bra_refs[d], bra_all.at[d], bra_sem.at[d]) for d in range(groups)
        ]
        for copy in ket_copies:
            copy.start()
        for copy in bra_copies:
            copy.start()
        for copy in ket_copies:
            copy.wait()
        for d in range(groups):
            for s in range(slots):
                row = pairs_ref[d * slots + s]
                safe = jnp.maximum(row, 0)
                for c in range(2):
                    stick = ket_all[c, safe]
                    chosen[c, s * part : (s + 1) * part] = jnp.where(row >= 0, stick, jnp.zeros_like(stick))
            bra_copies[d].wait()
            first = bra_all[d, 0].reshape(depth, bands).T
            second = bra_all[d, 1].reshape(depth, bands).T

            def dot(a, c):
                return jnp.dot(a, chosen[c], preferred_element_type=jnp.float32)

            real = dot(first, 0) + dot(second, 1)
            imag = dot(first, 1) - dot(second, 0)
            if d == 0:
                total[0] = real
                total[1] = imag
            else:
                total[0] += real
                total[1] += imag
        for d in range(groups):
            out = give_ref if d % 2 else keep_ref
            start = pl.multiple_of((me_ref[0] ^ d) * rows, rows)
            for c in range(2):
                out[d // 2, c] = total[c, pl.ds(start, rows)] * scale

    whole = pl.BlockSpec(memory_space=pltpu.VMEM)
    scalar = pl.BlockSpec(memory_space=pltpu.SMEM)
    far = pl.BlockSpec(memory_space=pl.ANY)
    half = jax.ShapeDtypeStruct((groups // 2, 2, rows, bands), jnp.float32)
    flops = 8 * groups * depth * bands * bands
    return pl.pallas_call(
        body,
        in_specs=[scalar, scalar] + [far] * (2 * groups),
        out_specs=[whole, whole],
        out_shape=[half, half],
        scratch_shapes=[
            pltpu.VMEM((groups, 2, slots, part, bands), jnp.bfloat16),
            pltpu.VMEM((2, groups * slots, part, bands), jnp.bfloat16),
            pltpu.VMEM((2, depth, bands), jnp.bfloat16),
            pltpu.VMEM((2, bands, bands), jnp.float32),
            pltpu.SemaphoreType.DMA((groups,)),
            pltpu.SemaphoreType.DMA((groups,)),
        ],
        cost_estimate=pl.CostEstimate(flops=flops, bytes_accessed=4 * groups * depth * bands, transcendentals=0),
    )(me.reshape(1), pairs, *bras, *kets)


def local(coefficients, stick_count, dest_device, dest_slot, source_stick):
    groups = lax.axis_size("ga")
    me = lax.axis_index("ga").astype(jnp.int32)
    _, slots, _, bands, waves = coefficients.shape
    scale = (2 * groups * slots * waves) ** (-0.5)
    pieces = pack(coefficients[0], groups, me)
    bras = [None] * groups
    bras[0] = pieces[0]
    for d in list(range(groups // 2, groups)) + list(range(1, groups // 2)):
        bras[d] = swapped_with(pieces[d], d)
    kets = [to_previous_pool(b) for b in bras]
    pairs = pair_list(stick_count, dest_device, dest_slot, source_stick, groups, slots, me)
    give, keep = multiply(bras, kets, pairs, me, groups, scale)
    distance = 1
    while True:
        keep = keep + swapped_with(give, distance)
        distance *= 2
        if distance == groups:
            break
        give, keep = keep[1::2], keep[0::2]
    return keep.reshape(1, 2, bands // groups, bands)


def solution(mesh):
    spec = P("pool", "ga")
    return jax.shard_map(
        local,
        mesh=mesh,
        in_specs=(P("pool", "ga", None, None, None), spec, spec, spec, spec),
        out_specs=P("pool", None, "ga", None),
        check_vma=False,
    )
```

```python
import jax
import jax.numpy as jnp
from jax import lax
from jax.experimental import pallas as pl
from jax.experimental.pallas import tpu as pltpu
from jax.sharding import PartitionSpec as P


def swapped_with(value, distance):
    count = lax.axis_size("ga")
    return lax.ppermute(value, "ga", [(i, i ^ distance) for i in range(count)])


def to_previous_pool(value):
    count = lax.axis_size("pool")
    return lax.ppermute(value, "pool", [(i, (i - 1) % count) for i in range(count)])


def pack(x, groups, me):
    slots, _, bands, waves = x.shape
    part = waves // groups
    if part % 16:
        cut = x.reshape(slots, 2, bands, groups, part).transpose(3, 1, 0, 4, 2)
        return [lax.dynamic_index_in_dim(cut, me ^ d, 0, False) for d in range(groups)]
    step = 4 if slots % 4 == 0 else 1

    def body(select_ref, x_ref, *refs):
        outs, held, sem = refs[:groups], refs[groups], refs[groups + 1]
        copies = [
            pltpu.make_async_copy(
                x_ref.at[pl.ds(i * step, step)], held.at[pl.ds(i * step, step)], sem.at[i]
            )
            for i in range(slots // step)
        ]
        for copy in copies:
            copy.start()
        for i, copy in enumerate(copies):
            copy.wait()
            for s in range(i * step, (i + 1) * step):
                for c in range(2):
                    turned = lax.dot_general(
                        select_ref[...],
                        held[s, c],
                        (((1,), (1,)), ((), ())),
                        preferred_element_type=jnp.float32,
                    ).astype(jnp.bfloat16)
                    for d in range(groups):
                        outs[d][c, s] = turned[d * part : (d + 1) * part]

    row = jnp.arange(waves, dtype=jnp.int32)
    source = ((row // part) ^ me) * part + row % part
    select = (source[:, None] == row[None, :]).astype(jnp.bfloat16)
    near = pl.BlockSpec(memory_space=pltpu.VMEM)
    return pl.pallas_call(
        body,
        in_specs=[near, pl.BlockSpec(memory_space=pl.ANY)],
        out_specs=[near] * groups,
        out_shape=[jax.ShapeDtypeStruct((2, slots, part, bands), jnp.bfloat16)] * groups,
        scratch_shapes=[
            pltpu.VMEM((slots, 2, bands, waves), jnp.bfloat16),
            pltpu.SemaphoreType.DMA((slots // step,)),
        ],
        compiler_params=pltpu.CompilerParams(vmem_limit_bytes=24 << 20),
        cost_estimate=pl.CostEstimate(
            flops=4 * slots * waves * waves * bands, bytes_accessed=x.size * 4, transcendentals=0
        ),
    )(select, x)


def gathered(mine, groups):
    rows = mine[None]
    levels = []
    distance = groups // 2
    while distance:
        other = swapped_with(rows, distance)
        rows = jnp.stack([rows, other], axis=len(levels))
        levels.append(2)
        rows = rows.reshape(*levels, 1, mine.shape[0])
        distance //= 2
    return rows.reshape(groups, mine.shape[0])


def pair_lists(bra_info, ket_info, groups, slots, me):
    counts = bra_info[:, 0]
    maps = ket_info[:, 1:].reshape(groups, 3, slots)
    device, slot, anchor = (maps[:, i].reshape(groups * slots) for i in range(3))
    number = jnp.arange(groups * slots, dtype=jnp.int32)
    here = ((number // slots) ^ me) * slots + number % slots
    lands = jnp.where(device >= 0, device * slots + slot, -1)
    live = (number % slots).reshape(groups, slots) < counts[:, None]
    agreeing = (anchor[:, None] == here[None, :]) & (lands[None, :] == here[:, None])
    agreeing &= live.reshape(-1)[:, None]
    ket_of = jnp.max(jnp.where(agreeing, number[None, :], -1), axis=1)
    bra_of = jnp.max(jnp.where(agreeing, number[:, None], -1), axis=0)
    return ket_of, bra_of


def multiply_plainly(bras, kets, ket_of, me, groups, scale):
    _, _, _, bands = bras[0].shape
    bra = jnp.concatenate(bras, axis=1)
    ket = jnp.concatenate(kets, axis=1)[:, jnp.maximum(ket_of, 0)]
    ket = jnp.where((ket_of >= 0)[None, :, None, None], ket, jnp.zeros_like(ket))

    def dot(a, b):
        return jnp.einsum("trm,trn->mn", bra[a], ket[b], preferred_element_type=jnp.float32)

    total = jnp.stack([dot(0, 0) + dot(1, 1), dot(0, 1) - dot(1, 0)]) * scale
    total = total.reshape(2, groups, bands // groups, bands).transpose(1, 0, 2, 3)
    total = total[jnp.arange(groups, dtype=jnp.int32) ^ me]
    return total[1::2], total[0::2]


def multiply(bras, kets, ket_of, bra_of, me, groups, scale):
    _, slots, part, bands = bras[0].shape
    rows = bands // groups
    depth = slots * part
    early = groups - 1
    near = pl.BlockSpec(memory_space=pltpu.VMEM)
    scalar = pl.BlockSpec(memory_space=pltpu.SMEM)

    def turned(chosen, d):
        first = chosen[0, d * slots : (d + 1) * slots].reshape(depth, bands).T
        second = chosen[1, d * slots : (d + 1) * slots].reshape(depth, bands).T
        upper = jnp.concatenate([first, second], axis=1)
        lower = jnp.concatenate([-second, first], axis=1)
        return jnp.concatenate([upper, lower], axis=0)

    def flat(ket_ref):
        return ket_ref[...].reshape(2 * depth, bands)

    def most(ket_of_ref, bra_of_ref, *refs):
        bra_refs, ket_refs = refs[:groups], refs[groups : groups + early]
        total_ref, last_ref, chosen = refs[groups + early :]
        for d in range(groups):

            def put(s, _, d=d):
                row = ket_of_ref[d * slots + s]
                row = jnp.where(row >= 0, row, groups * slots)
                for c in range(2):
                    chosen[c, row] = bra_refs[d][c, s]
                return 0

            lax.fori_loop(0, slots, put, 0, unroll=8)

        def clear(row, _):
            @pl.when(bra_of_ref[row] < 0)
            def _():
                for c in range(2):
                    chosen[c, row] = jnp.zeros((part, bands), jnp.bfloat16)

            return 0

        lax.fori_loop(0, groups * slots, clear, 0, unroll=8)
        for d in range(early):
            product = jnp.dot(turned(chosen, d), flat(ket_refs[d]), preferred_element_type=jnp.float32)
            if d == 0:
                total_ref[...] = product
            else:
                total_ref[...] += product
        last_ref[...] = turned(chosen, early)

    def rest(me_ref, total_ref, last_ref, ket_ref, give_ref, keep_ref, sums):
        sums[...] = total_ref[...] + jnp.dot(
            last_ref[...], flat(ket_ref), preferred_element_type=jnp.float32
        )
        for d in range(groups):
            out = give_ref if d % 2 else keep_ref
            start = (me_ref[0] ^ d) * rows
            for c in range(2):
                out[d // 2, c] = sums[pl.ds(pl.multiple_of(c * bands + start, rows), rows)] * scale

    flops = 8 * depth * bands * bands
    total, last = pl.pallas_call(
        most,
        in_specs=[scalar, scalar] + [near] * (groups + early),
        out_specs=[near, near],
        out_shape=[
            jax.ShapeDtypeStruct((2 * bands, bands), jnp.float32),
            jax.ShapeDtypeStruct((2 * bands, 2 * depth), jnp.bfloat16),
        ],
        scratch_shapes=[pltpu.VMEM((2, groups * slots + 1, part, bands), jnp.bfloat16)],
        compiler_params=pltpu.CompilerParams(vmem_limit_bytes=32 << 20),
        cost_estimate=pl.CostEstimate(flops=early * flops, bytes_accessed=1 << 20, transcendentals=0),
    )(ket_of, bra_of, *bras, *kets[:early])
    half = jax.ShapeDtypeStruct((groups // 2, 2, rows, bands), jnp.float32)
    return pl.pallas_call(
        rest,
        in_specs=[scalar, near, near, near],
        out_specs=[near, near],
        out_shape=[half, half],
        scratch_shapes=[pltpu.VMEM((2 * bands, bands), jnp.float32)],
        compiler_params=pltpu.CompilerParams(vmem_limit_bytes=16 << 20),
        cost_estimate=pl.CostEstimate(flops=flops, bytes_accessed=1 << 20, transcendentals=0),
    )(me.reshape(1), total, last, kets[early])


def local(coefficients, stick_count, dest_device, dest_slot, source_stick):
    groups = lax.axis_size("ga")
    me = lax.axis_index("ga").astype(jnp.int32)
    _, slots, _, bands, waves = coefficients.shape
    scale = (2 * groups * slots * waves) ** (-0.5)
    pieces = pack(coefficients[0], groups, me)
    mine = jnp.concatenate([stick_count, dest_device, dest_slot, source_stick], axis=1)[0]
    bra_info = gathered(mine, groups)
    ket_info = to_previous_pool(bra_info)
    bras, kets = [None] * groups, [None] * groups
    bras[0] = pieces[0]
    for d in [0, *range(1, groups // 2), *range(groups // 2, groups)]:
        if d:
            bras[d] = swapped_with(pieces[d], d)
            bras[d], previous = lax.optimization_barrier((bras[d], bras[d - 1]))
        kets[d] = to_previous_pool(bras[d])
    ket_of, bra_of = pair_lists(bra_info, ket_info, groups, slots, me)
    if (waves // groups) % 16:
        give, keep = multiply_plainly(bras, kets, ket_of, me, groups, scale)
    else:
        give, keep = multiply(bras, kets, ket_of, bra_of, me, groups, scale)
    distance = 1
    while True:
        keep = keep + swapped_with(give, distance)
        distance *= 2
        if distance == groups:
            break
        give, keep = keep[1::2], keep[0::2]
    return keep.reshape(1, 2, bands // groups, bands)


def solution(mesh):
    spec = P("pool", "ga")
    return jax.shard_map(
        local,
        mesh=mesh,
        in_specs=(P("pool", "ga", None, None, None), spec, spec, spec, spec),
        out_specs=P("pool", None, "ga", None),
        check_vma=False,
    )
```

```python
import jax
import jax.numpy as jnp
from jax import lax
from jax.experimental import pallas as pl
from jax.experimental.pallas import tpu as pltpu
from jax.sharding import PartitionSpec as P


def swapped_with(value, distance):
    count = lax.axis_size("ga")
    return lax.ppermute(value, "ga", [(i, i ^ distance) for i in range(count)])


def to_previous_pool(value):
    count = lax.axis_size("pool")
    return lax.ppermute(value, "pool", [(i, (i - 1) % count) for i in range(count)])


def pack(x, groups, me):
    slots, _, bands, waves = x.shape
    part = waves // groups
    if part % 16:
        cut = x.reshape(slots, 2, bands, groups, part).transpose(3, 1, 0, 4, 2)
        return [lax.dynamic_index_in_dim(cut, me ^ d, 0, False) for d in range(groups)]
    step = 4 if slots % 4 == 0 else 1

    def body(select_ref, x_ref, *refs):
        outs, held, sem = refs[:groups], refs[groups], refs[groups + 1]
        copies = [
            pltpu.make_async_copy(
                x_ref.at[pl.ds(i * step, step)], held.at[pl.ds(i * step, step)], sem.at[i]
            )
            for i in range(slots // step)
        ]
        for copy in copies:
            copy.start()
        for i, copy in enumerate(copies):
            copy.wait()
            for s in range(i * step, (i + 1) * step):
                for c in range(2):
                    turned = lax.dot_general(
                        select_ref[...],
                        held[s, c],
                        (((1,), (1,)), ((), ())),
                        preferred_element_type=jnp.float32,
                    ).astype(jnp.bfloat16)
                    for d in range(groups):
                        outs[d][c, s] = turned[d * part : (d + 1) * part]

    row = jnp.arange(waves, dtype=jnp.int32)
    source = ((row // part) ^ me) * part + row % part
    select = (source[:, None] == row[None, :]).astype(jnp.bfloat16)
    near = pl.BlockSpec(memory_space=pltpu.VMEM)
    return pl.pallas_call(
        body,
        in_specs=[near, pl.BlockSpec(memory_space=pltpu.HBM)],
        out_specs=[near] * groups,
        out_shape=[jax.ShapeDtypeStruct((2, slots, part, bands), jnp.bfloat16)] * groups,
        scratch_shapes=[
            pltpu.VMEM((slots, 2, bands, waves), jnp.bfloat16),
            pltpu.SemaphoreType.DMA((slots // step,)),
        ],
        compiler_params=pltpu.CompilerParams(vmem_limit_bytes=24 << 20),
        cost_estimate=pl.CostEstimate(
            flops=4 * slots * waves * waves * bands, bytes_accessed=x.size * 4, transcendentals=0
        ),
    )(select, x)


def passed_around(mine, groups):
    rows = [mine]
    for d in range(2, groups, 2):
        rows.append(swapped_with(mine, d))
    return rows


def pair_lists(bra_info, ket_info, groups, slots, me):
    counts = bra_info[:, 0]
    maps = ket_info[:, 1:].reshape(groups, 3, slots)
    device, slot, anchor = (maps[:, i].reshape(groups * slots) for i in range(3))
    number = jnp.arange(groups * slots, dtype=jnp.int32)
    here = ((number // slots) ^ me) * slots + number % slots
    lands = jnp.where(device >= 0, device * slots + slot, -1)
    live = (number % slots).reshape(groups, slots) < counts[:, None]
    agreeing = (anchor[:, None] == here[None, :]) & (lands[None, :] == here[:, None])
    agreeing &= live.reshape(-1)[:, None]
    ket_of = jnp.max(jnp.where(agreeing, number[None, :], -1), axis=1)
    bra_of = jnp.max(jnp.where(agreeing, number[:, None], -1), axis=0)
    return ket_of, bra_of


def multiply_plainly(bras, kets, ket_of, me, groups, scale):
    _, _, _, bands = bras[0].shape
    bra = jnp.concatenate(bras, axis=1)
    ket = jnp.concatenate(kets, axis=1)[:, jnp.maximum(ket_of, 0)]
    ket = jnp.where((ket_of >= 0)[None, :, None, None], ket, jnp.zeros_like(ket))

    def dot(a, b):
        return jnp.einsum("trm,trn->mn", bra[a], ket[b], preferred_element_type=jnp.float32)

    total = jnp.stack([dot(0, 0) + dot(1, 1), dot(0, 1) - dot(1, 0)]) * scale
    total = total.reshape(2, groups, bands // groups, bands).transpose(1, 0, 2, 3)
    total = total[jnp.arange(groups, dtype=jnp.int32) ^ me]
    return total[1::2], total[0::2]


def multiply(bras, kets, ket_of, bra_of, me, groups, scale):
    _, slots, part, bands = bras[0].shape
    rows = bands // groups
    depth = slots * part
    early = groups - 1
    near = pl.BlockSpec(memory_space=pltpu.VMEM)
    scalar = pl.BlockSpec(memory_space=pltpu.SMEM)

    def turned(chosen, d):
        first = chosen[0, d * slots : (d + 1) * slots].reshape(depth, bands).T
        second = chosen[1, d * slots : (d + 1) * slots].reshape(depth, bands).T
        upper = jnp.concatenate([first, second], axis=1)
        lower = jnp.concatenate([-second, first], axis=1)
        return jnp.concatenate([upper, lower], axis=0)

    def flat(ket_ref):
        return ket_ref[...].reshape(2 * depth, bands)

    def most(ket_of_ref, bra_of_ref, *refs):
        bra_refs, ket_refs = refs[:groups], refs[groups : groups + early]
        total_ref, last_ref, chosen = refs[groups + early :]
        for d in range(groups):

            def put(s, _, d=d):
                row = ket_of_ref[d * slots + s]
                row = jnp.where(row >= 0, row, groups * slots)
                for c in range(2):
                    chosen[c, row] = bra_refs[d][c, s]
                return 0

            lax.fori_loop(0, slots, put, 0, unroll=8)

        def clear(row, _):
            @pl.when(bra_of_ref[row] < 0)
            def _():
                for c in range(2):
                    chosen[c, row] = jnp.zeros((part, bands), jnp.bfloat16)

            return 0

        lax.fori_loop(0, groups * slots, clear, 0, unroll=8)
        for d in range(early):
            product = jnp.dot(turned(chosen, d), flat(ket_refs[d]), preferred_element_type=jnp.float32)
            if d == 0:
                total_ref[...] = product
            else:
                total_ref[...] += product
        last_ref[...] = turned(chosen, early)

    def rest(me_ref, total_ref, last_ref, ket_ref, give_ref, keep_ref, sums):
        sums[...] = total_ref[...] + jnp.dot(
            last_ref[...], flat(ket_ref), preferred_element_type=jnp.float32
        )
        for d in range(groups):
            out = give_ref if d % 2 else keep_ref
            start = (me_ref[0] ^ d) * rows
            for c in range(2):
                out[d // 2, c] = sums[pl.ds(pl.multiple_of(c * bands + start, rows), rows)] * scale

    flops = 8 * depth * bands * bands
    total, last = pl.pallas_call(
        most,
        in_specs=[scalar, scalar] + [near] * (groups + early),
        out_specs=[near, near],
        out_shape=[
            jax.ShapeDtypeStruct((2 * bands, bands), jnp.float32),
            jax.ShapeDtypeStruct((2 * bands, 2 * depth), jnp.bfloat16),
        ],
        scratch_shapes=[pltpu.VMEM((2, groups * slots + 1, part, bands), jnp.bfloat16)],
        compiler_params=pltpu.CompilerParams(vmem_limit_bytes=32 << 20),
        cost_estimate=pl.CostEstimate(flops=early * flops, bytes_accessed=1 << 20, transcendentals=0),
    )(ket_of, bra_of, *bras, *kets[:early])
    half = jax.ShapeDtypeStruct((groups // 2, 2, rows, bands), jnp.float32)
    return pl.pallas_call(
        rest,
        in_specs=[scalar, near, near, near],
        out_specs=[near, near],
        out_shape=[half, half],
        scratch_shapes=[pltpu.VMEM((2 * bands, bands), jnp.float32)],
        compiler_params=pltpu.CompilerParams(vmem_limit_bytes=16 << 20),
        cost_estimate=pl.CostEstimate(flops=flops, bytes_accessed=1 << 20, transcendentals=0),
    )(me.reshape(1), total, last, kets[early])


def zero_like(value):
    def body(_, out_ref):
        out_ref[0, 0] = 0

    scalar = pl.BlockSpec(memory_space=pltpu.SMEM)
    return pl.pallas_call(
        body,
        in_specs=[scalar],
        out_specs=scalar,
        out_shape=jax.ShapeDtypeStruct((1, 1), jnp.int32),
        compiler_params=pltpu.CompilerParams(vmem_limit_bytes=1 << 20),
    )(value)


def local(coefficients, stick_count, dest_device, dest_slot, source_stick):
    groups = lax.axis_size("ga")
    me = lax.axis_index("ga").astype(jnp.int32)
    _, slots, _, bands, waves = coefficients.shape
    scale = (2 * groups * slots * waves) ** (-0.5)
    pieces = pack(coefficients[0], groups, me)
    mine = jnp.concatenate([stick_count, dest_device, dest_slot, source_stick], axis=1)[0]
    info = passed_around(mine, groups)
    bras, kets = [None] * groups, [None] * groups
    bras[0] = pieces[0]
    arrivals = interleaved(range(1, groups // 2), range(groups // 2, groups))
    kets[0] = to_previous_pool(bras[0])
    anchor = me.reshape(1, 1)
    for place, d in enumerate(arrivals):
        bras[d] = swapped_with(pieces[d], d)
        kets[d] = to_previous_pool(bras[d])
        if place == len(arrivals) - 1:
            break
        anchor = zero_like(anchor)
        if place == len(arrivals) - 2:
            before_last = anchor
        if place == groups // 2:
            even = jnp.stack(info) + anchor
    odd = swapped_with(even, 1)
    bra_info = jnp.stack([even, odd], axis=1).reshape(groups, mine.shape[0])
    ket_info = to_previous_pool(bra_info)
    ket_of, bra_of = pair_lists(bra_info, ket_info + before_last, groups, slots, me)
    if (waves // groups) % 16:
        give, keep = multiply_plainly(bras, kets, ket_of, me, groups, scale)
    else:
        give, keep = multiply(bras, kets, ket_of, bra_of, me, groups, scale)
    distance = 1
    while True:
        keep = keep + swapped_with(give, distance)
        distance *= 2
        if distance == groups:
            break
        give, keep = keep[1::2], keep[0::2]
    return keep.reshape(1, 2, bands // groups, bands)


def interleaved(first, second):
    first, second = list(first), list(second)
    mixed = [item for pair in zip(first, second) for item in pair]
    return mixed + second[len(first) :]


def solution(mesh):
    spec = P("pool", "ga")
    return jax.shard_map(
        local,
        mesh=mesh,
        in_specs=(P("pool", "ga", None, None, None), spec, spec, spec, spec),
        out_specs=P("pool", None, "ga", None),
        check_vma=False,
    )
```

```python
import jax
import jax.numpy as jnp
from jax import lax
from jax.experimental import pallas as pl
from jax.experimental.pallas import tpu as pltpu
from jax.sharding import PartitionSpec as P


def swapped_with(value, distance):
    count = lax.axis_size("ga")
    return lax.ppermute(value, "ga", [(i, i ^ distance) for i in range(count)])


def to_previous_pool(value):
    count = lax.axis_size("pool")
    return lax.ppermute(value, "pool", [(i, (i - 1) % count) for i in range(count)])


def pack(x, groups, me):
    slots, _, bands, waves = x.shape
    part = waves // groups
    if part % 16:
        cut = x.reshape(slots, 2, bands, groups, part).transpose(3, 1, 0, 4, 2)
        return [lax.dynamic_index_in_dim(cut, me ^ d, 0, False) for d in range(groups)]
    step = 4 if slots % 4 == 0 else 1

    def body(select_ref, x_ref, *outs):
        place = pl.program_id(0) * step
        for s in range(step):
            for c in range(2):
                turned = lax.dot_general(
                    select_ref[...],
                    x_ref[s, c],
                    (((1,), (1,)), ((), ())),
                    preferred_element_type=jnp.float32,
                ).astype(jnp.bfloat16)
                for d in range(groups):
                    outs[d][c, place + s] = turned[d * part : (d + 1) * part]

    row = jnp.arange(waves, dtype=jnp.int32)
    source = ((row // part) ^ me) * part + row % part
    select = (source[:, None] == row[None, :]).astype(jnp.bfloat16)
    near = pl.BlockSpec(memory_space=pltpu.VMEM)
    return pl.pallas_call(
        body,
        grid=(slots // step,),
        in_specs=[near, pl.BlockSpec((step, 2, bands, waves), lambda i: (i, 0, 0, 0))],
        out_specs=[near] * groups,
        out_shape=[jax.ShapeDtypeStruct((2, slots, part, bands), jnp.bfloat16)] * groups,
        compiler_params=pltpu.CompilerParams(vmem_limit_bytes=48 << 20),
        cost_estimate=pl.CostEstimate(
            flops=4 * slots * waves * waves * bands, bytes_accessed=x.size * 4, transcendentals=0
        ),
    )(select, x)


def passed_around(mine, groups):
    rows = [mine]
    for d in range(1, groups):
        rows.append(swapped_with(mine, d))
    return rows


def pair_list(bra_info, ket_info, groups, slots, me):
    counts = bra_info[:, 0]
    maps = ket_info[:, 1:].reshape(groups, 3, slots)
    device, slot, anchor = (maps[:, i].reshape(groups * slots) for i in range(3))
    number = jnp.arange(groups * slots, dtype=jnp.int32)
    here = ((number // slots) ^ me) * slots + number % slots
    lands = jnp.where(device >= 0, device * slots + slot, -1)
    live = (number % slots).reshape(groups, slots) < counts[:, None]
    agreeing = (anchor[:, None] == here[None, :]) & (lands[None, :] == here[:, None])
    agreeing &= live.reshape(-1)[:, None]
    return jnp.max(jnp.where(agreeing, number[None, :], -1), axis=1)


def multiply_plainly(bras, kets, ket_of, me, groups, scale):
    _, _, _, bands = bras[0].shape
    bra = jnp.concatenate(bras, axis=1)
    ket = jnp.concatenate(kets, axis=1)[:, jnp.maximum(ket_of, 0)]
    ket = jnp.where((ket_of >= 0)[None, :, None, None], ket, jnp.zeros_like(ket))

    def dot(a, b):
        return jnp.einsum("trm,trn->mn", bra[a], ket[b], preferred_element_type=jnp.float32)

    total = jnp.stack([dot(0, 0) + dot(1, 1), dot(0, 1) - dot(1, 0)]) * scale
    total = total.reshape(2, groups, bands // groups, bands).transpose(1, 0, 2, 3)
    total = total[jnp.arange(groups, dtype=jnp.int32) ^ me]
    return total[1::2], total[0::2]


def multiply(bras, kets, ket_of, me, groups, scale):
    _, slots, part, bands = bras[0].shape
    rows = bands // groups
    depth = slots * part
    early = groups - 1
    near = pl.BlockSpec(memory_space=pltpu.VMEM)
    scalar = pl.BlockSpec(memory_space=pltpu.SMEM)

    def turned(chosen, d):
        first = chosen[0, d * slots : (d + 1) * slots].reshape(depth, bands).T
        second = chosen[1, d * slots : (d + 1) * slots].reshape(depth, bands).T
        upper = jnp.concatenate([first, second], axis=1)
        lower = jnp.concatenate([-second, first], axis=1)
        return jnp.concatenate([upper, lower], axis=0)

    def flat(ket_ref):
        return ket_ref[...].reshape(2 * depth, bands)

    def most(ket_of_ref, *refs):
        bra_refs, ket_refs = refs[:groups], refs[groups : groups + early]
        total_ref, last_ref, chosen = refs[groups + early :]
        chosen[...] = jnp.zeros_like(chosen)
        for d in range(groups):

            def put(s, _, d=d):
                row = ket_of_ref[d * slots + s]
                row = jnp.where(row >= 0, row, groups * slots)
                for c in range(2):
                    chosen[c, row] = bra_refs[d][c, s]
                return 0

            lax.fori_loop(0, slots, put, 0, unroll=8)
        for d in range(early):
            product = jnp.dot(turned(chosen, d), flat(ket_refs[d]), preferred_element_type=jnp.float32)
            if d == 0:
                total_ref[...] = product
            else:
                total_ref[...] += product
        last_ref[...] = turned(chosen, early)

    def rest(me_ref, total_ref, last_ref, ket_ref, give_ref, keep_ref, sums):
        sums[...] = total_ref[...] + jnp.dot(
            last_ref[...], flat(ket_ref), preferred_element_type=jnp.float32
        )
        for d in range(groups):
            out = give_ref if d % 2 else keep_ref
            start = (me_ref[0] ^ d) * rows
            for c in range(2):
                out[d // 2, c] = sums[pl.ds(pl.multiple_of(c * bands + start, rows), rows)] * scale

    flops = 8 * depth * bands * bands
    total, last = pl.pallas_call(
        most,
        in_specs=[scalar] + [near] * (groups + early),
        out_specs=[near, near],
        out_shape=[
            jax.ShapeDtypeStruct((2 * bands, bands), jnp.float32),
            jax.ShapeDtypeStruct((2 * bands, 2 * depth), jnp.bfloat16),
        ],
        scratch_shapes=[pltpu.VMEM((2, groups * slots + 1, part, bands), jnp.bfloat16)],
        compiler_params=pltpu.CompilerParams(vmem_limit_bytes=32 << 20),
        cost_estimate=pl.CostEstimate(flops=early * flops, bytes_accessed=1 << 20, transcendentals=0),
    )(ket_of, *bras, *kets[:early])
    half = jax.ShapeDtypeStruct((groups // 2, 2, rows, bands), jnp.float32)
    return pl.pallas_call(
        rest,
        in_specs=[scalar, near, near, near],
        out_specs=[near, near],
        out_shape=[half, half],
        scratch_shapes=[pltpu.VMEM((2 * bands, bands), jnp.float32)],
        compiler_params=pltpu.CompilerParams(vmem_limit_bytes=16 << 20),
        cost_estimate=pl.CostEstimate(flops=flops, bytes_accessed=1 << 20, transcendentals=0),
    )(me.reshape(1), total, last, kets[early])


def zero_like(value):
    def body(_, out_ref):
        out_ref[0, 0] = 0

    scalar = pl.BlockSpec(memory_space=pltpu.SMEM)
    return pl.pallas_call(
        body,
        in_specs=[scalar],
        out_specs=scalar,
        out_shape=jax.ShapeDtypeStruct((1, 1), jnp.int32),
        compiler_params=pltpu.CompilerParams(vmem_limit_bytes=1 << 20),
    )(value)


def local(coefficients, stick_count, dest_device, dest_slot, source_stick):
    groups = lax.axis_size("ga")
    me = lax.axis_index("ga").astype(jnp.int32)
    _, slots, _, bands, waves = coefficients.shape
    scale = (2 * groups * slots * waves) ** (-0.5)
    pieces = pack(coefficients[0], groups, me)
    mine = jnp.concatenate([stick_count, dest_device, dest_slot, source_stick], axis=1)[0]
    info = passed_around(mine, groups)
    bras, kets = [None] * groups, [None] * groups
    bras[0] = pieces[0]
    arrivals = interleaved(range(1, groups // 2), range(groups // 2, groups))
    kets[0] = to_previous_pool(bras[0])
    anchor = me.reshape(1, 1)
    for place, d in enumerate(arrivals):
        bras[d] = swapped_with(pieces[d], d)
        kets[d] = to_previous_pool(bras[d])
        if place == len(arrivals) - 1:
            break
        anchor = zero_like(anchor)
        if place == len(arrivals) - 2:
            before_last = anchor
        if place == 2:
            bra_info = jnp.stack(info) + anchor
    ket_info = to_previous_pool(bra_info)
    ket_of = pair_list(bra_info, ket_info + before_last, groups, slots, me)
    if (waves // groups) % 16:
        give, keep = multiply_plainly(bras, kets, ket_of, me, groups, scale)
    else:
        give, keep = multiply(bras, kets, ket_of, me, groups, scale)
    distance = 1
    while True:
        keep = keep + swapped_with(give, distance)
        distance *= 2
        if distance == groups:
            break
        give, keep = keep[1::2], keep[0::2]
    return keep.reshape(1, 2, bands // groups, bands)


def interleaved(first, second):
    first, second = list(first), list(second)
    mixed = [item for pair in zip(first, second) for item in pair]
    return mixed + second[len(first) :]


def solution(mesh):
    spec = P("pool", "ga")
    return jax.shard_map(
        local,
        mesh=mesh,
        in_specs=(P("pool", "ga", None, None, None), spec, spec, spec, spec),
        out_specs=P("pool", None, "ga", None),
        check_vma=False,
    )
```

```python
import jax
import jax.numpy as jnp
from jax import lax
from jax.experimental import pallas as pl
from jax.experimental.pallas import tpu as pltpu
from jax.sharding import PartitionSpec as P


def swapped_with(value, distance):
    count = lax.axis_size("ga")
    return lax.ppermute(value, "ga", [(i, i ^ distance) for i in range(count)])


def to_previous_pool(value):
    count = lax.axis_size("pool")
    return lax.ppermute(value, "pool", [(i, (i - 1) % count) for i in range(count)])


def pack(x, groups, me):
    slots, _, bands, waves = x.shape
    part = waves // groups
    if part % 16:
        cut = x.reshape(slots, 2, bands, groups, part).transpose(3, 1, 0, 4, 2)
        return [lax.dynamic_index_in_dim(cut, me ^ d, 0, False) for d in range(groups)]
    step = 4 if slots % 4 == 0 else 1

    def body(select_ref, x_ref, *refs):
        outs, held, sem = refs[:groups], refs[groups], refs[groups + 1]
        copies = [
            pltpu.make_async_copy(
                x_ref.at[pl.ds(i * step, step)], held.at[pl.ds(i * step, step)], sem.at[i]
            )
            for i in range(slots // step)
        ]
        for copy in copies:
            copy.start()
        for i, copy in enumerate(copies):
            copy.wait()
            for s in range(i * step, (i + 1) * step):
                for c in range(2):
                    turned = lax.dot_general(
                        select_ref[...],
                        held[s, c],
                        (((1,), (1,)), ((), ())),
                        preferred_element_type=jnp.float32,
                    ).astype(jnp.bfloat16)
                    for d in range(groups):
                        outs[d][c, s] = turned[d * part : (d + 1) * part]

    row = jnp.arange(waves, dtype=jnp.int32)
    source = ((row // part) ^ me) * part + row % part
    select = (source[:, None] == row[None, :]).astype(jnp.bfloat16)
    near = pl.BlockSpec(memory_space=pltpu.VMEM)
    return pl.pallas_call(
        body,
        in_specs=[near, pl.BlockSpec(memory_space=pltpu.HBM)],
        out_specs=[near] * groups,
        out_shape=[jax.ShapeDtypeStruct((2, slots, part, bands), jnp.bfloat16)] * groups,
        scratch_shapes=[
            pltpu.VMEM((slots, 2, bands, waves), jnp.bfloat16),
            pltpu.SemaphoreType.DMA((slots // step,)),
        ],
        compiler_params=pltpu.CompilerParams(vmem_limit_bytes=48 << 20),
        cost_estimate=pl.CostEstimate(
            flops=4 * slots * waves * waves * bands, bytes_accessed=x.size * 4, transcendentals=0
        ),
    )(select, x)


def passed_around(mine, groups):
    rows = [mine]
    for d in range(1, groups):
        rows.append(swapped_with(mine, d))
    return rows


def pair_list(bra_info, ket_info, groups, slots, me):
    counts = bra_info[:, 0]
    maps = ket_info[:, 1:].reshape(groups, 3, slots)
    device, slot, anchor = (maps[:, i].reshape(groups * slots) for i in range(3))
    number = jnp.arange(groups * slots, dtype=jnp.int32)
    here = ((number // slots) ^ me) * slots + number % slots
    lands = jnp.where(device >= 0, device * slots + slot, -1)
    live = (number % slots).reshape(groups, slots) < counts[:, None]
    agreeing = (anchor[:, None] == here[None, :]) & (lands[None, :] == here[:, None])
    agreeing &= live.reshape(-1)[:, None]
    return jnp.max(jnp.where(agreeing, number[None, :], -1), axis=1)


def multiply_plainly(bras, kets, ket_of, me, groups, scale):
    _, _, _, bands = bras[0].shape
    bra = jnp.concatenate(bras, axis=1)
    ket = jnp.concatenate(kets, axis=1)[:, jnp.maximum(ket_of, 0)]
    ket = jnp.where((ket_of >= 0)[None, :, None, None], ket, jnp.zeros_like(ket))

    def dot(a, b):
        return jnp.einsum("trm,trn->mn", bra[a], ket[b], preferred_element_type=jnp.float32)

    total = jnp.stack([dot(0, 0) + dot(1, 1), dot(0, 1) - dot(1, 0)]) * scale
    total = total.reshape(2, groups, bands // groups, bands)
    total = total[:, jnp.arange(groups, dtype=jnp.int32) ^ me]
    plan = halving_plan(groups)
    return [total[c][jnp.array(blocks)] for c in range(2) for blocks in plan[c][0]]


def multiply(bras, kets, ket_of, me, groups, scale):
    _, slots, part, bands = bras[0].shape
    rows = bands // groups
    depth = slots * part
    early = groups - 1
    near = pl.BlockSpec(memory_space=pltpu.VMEM)
    scalar = pl.BlockSpec(memory_space=pltpu.SMEM)

    def turned(chosen, d):
        first = chosen[0, d * slots : (d + 1) * slots].reshape(depth, bands).T
        second = chosen[1, d * slots : (d + 1) * slots].reshape(depth, bands).T
        upper = jnp.concatenate([first, second], axis=1)
        lower = jnp.concatenate([-second, first], axis=1)
        return jnp.concatenate([upper, lower], axis=0)

    def flat(ket_ref):
        return ket_ref[...].reshape(2 * depth, bands)

    def most(ket_of_ref, *refs):
        bra_refs, ket_refs = refs[:groups], refs[groups : groups + early]
        total_ref, last_ref, chosen = refs[groups + early :]
        chosen[...] = jnp.zeros_like(chosen)
        for d in range(groups):

            def put(s, _, d=d):
                row = ket_of_ref[d * slots + s]
                row = jnp.where(row >= 0, row, groups * slots)
                for c in range(2):
                    chosen[c, row] = bra_refs[d][c, s]
                return 0

            lax.fori_loop(0, slots, put, 0, unroll=8)
        for d in range(early):
            product = jnp.dot(turned(chosen, d), flat(ket_refs[d]), preferred_element_type=jnp.float32)
            if d == 0:
                total_ref[...] = product
            else:
                total_ref[...] += product
        last_ref[...] = turned(chosen, early)

    plan = halving_plan(groups)

    def rest(me_ref, total_ref, last_ref, ket_ref, *refs):
        outs, sums = refs[:-1], refs[-1]
        sums[...] = total_ref[...] + jnp.dot(
            last_ref[...], flat(ket_ref), preferred_element_type=jnp.float32
        )
        for c in range(2):
            for out, blocks in zip(outs[2 * c : 2 * c + 2], plan[c][0]):
                for place, d in enumerate(blocks):
                    start = c * bands + (me_ref[0] ^ d) * rows
                    out[place] = sums[pl.ds(pl.multiple_of(start, rows), rows)] * scale

    flops = 8 * depth * bands * bands
    total, last = pl.pallas_call(
        most,
        in_specs=[scalar] + [near] * (groups + early),
        out_specs=[near, near],
        out_shape=[
            jax.ShapeDtypeStruct((2 * bands, bands), jnp.float32),
            jax.ShapeDtypeStruct((2 * bands, 2 * depth), jnp.bfloat16),
        ],
        scratch_shapes=[pltpu.VMEM((2, groups * slots + 1, part, bands), jnp.bfloat16)],
        compiler_params=pltpu.CompilerParams(vmem_limit_bytes=32 << 20),
        cost_estimate=pl.CostEstimate(flops=early * flops, bytes_accessed=1 << 20, transcendentals=0),
    )(ket_of, *bras, *kets[:early])
    half = jax.ShapeDtypeStruct((groups // 2, rows, bands), jnp.float32)
    return pl.pallas_call(
        rest,
        in_specs=[scalar, near, near, near],
        out_specs=[near] * 4,
        out_shape=[half] * 4,
        scratch_shapes=[pltpu.VMEM((2 * bands, bands), jnp.float32)],
        compiler_params=pltpu.CompilerParams(vmem_limit_bytes=16 << 20),
        cost_estimate=pl.CostEstimate(flops=flops, bytes_accessed=1 << 20, transcendentals=0),
    )(me.reshape(1), total, last, kets[early])


def halving_plan(groups):
    bits = groups.bit_length() - 1
    plans = []
    for order in ([*range(bits)], [1, 0, *range(2, bits)]):
        blocks, steps = list(range(groups)), []
        for bit in order:
            kept = [i for i in blocks if not i >> bit & 1]
            steps.append(([i | 1 << bit for i in kept], kept))
            blocks = kept
        plans.append((steps[0], order, steps))
    return plans


def reduce_to_owner(parts, groups):
    plan = halving_plan(groups)
    gives, keeps = [parts[0], parts[2]], [parts[1], parts[3]]
    _, rows, bands = gives[0].shape
    steps = groups.bit_length() - 1
    near = pl.BlockSpec(memory_space=pltpu.VMEM)
    for step in range(steps):
        bits = [plan[c][1][step] for c in range(2)]
        if bits[0] == bits[1] and len(gives) == 1:
            got = [swapped_with(gives[0], 1 << bits[0])]
        else:
            got = [swapped_with(gives[c], 1 << bits[c]) for c in range(2)]
        if step == steps - 1:
            break
        joined = plan[0][1][step + 1] == plan[1][1][step + 1]
        count = groups >> (step + 2)

        def body(*refs, step=step, joined=joined, count=count, number=len(got)):
            held, come, outs = refs[:number], refs[number : 2 * number], refs[2 * number :]
            for c in range(2):
                steps_of = plan[c][2]
                now = steps_of[step][1]
                for kind in range(2):
                    for place, block in enumerate(steps_of[step + 1][kind]):
                        at = now.index(block)
                        source = (c, at) if number == 1 else (at,)
                        which = 0 if number == 1 else c
                        value = held[which][source] + come[which][source]
                        if joined:
                            outs[kind][c, place] = value
                        else:
                            outs[2 * c + kind][place] = value

        if joined:
            shapes = [jax.ShapeDtypeStruct((2, count, rows, bands), jnp.float32)] * 2
        else:
            shapes = [jax.ShapeDtypeStruct((count, rows, bands), jnp.float32)] * 4
        outs = pl.pallas_call(
            body,
            in_specs=[near] * (2 * len(got)),
            out_specs=[near] * len(shapes),
            out_shape=shapes,
            compiler_params=pltpu.CompilerParams(vmem_limit_bytes=8 << 20),
        )(*keeps, *got)
        gives, keeps = outs[0::2], outs[1::2]
    if len(keeps) == 1:
        return (keeps[0] + got[0])[:, 0]
    return jnp.stack([(keep + come)[0] for keep, come in zip(keeps, got)])


def zero_like(value):
    def body(_, out_ref):
        out_ref[0, 0] = 0

    scalar = pl.BlockSpec(memory_space=pltpu.SMEM)
    return pl.pallas_call(
        body,
        in_specs=[scalar],
        out_specs=scalar,
        out_shape=jax.ShapeDtypeStruct((1, 1), jnp.int32),
        compiler_params=pltpu.CompilerParams(vmem_limit_bytes=1 << 20),
    )(value)


def local(coefficients, stick_count, dest_device, dest_slot, source_stick):
    groups = lax.axis_size("ga")
    me = lax.axis_index("ga").astype(jnp.int32)
    _, slots, _, _, waves = coefficients.shape
    scale = (2 * groups * slots * waves) ** (-0.5)
    pieces = pack(coefficients[0], groups, me)
    mine = jnp.concatenate([stick_count, dest_device, dest_slot, source_stick], axis=1)[0]
    info = passed_around(mine, groups)
    bras, kets = [None] * groups, [None] * groups
    bras[0] = pieces[0]
    arrivals = arrival_order(groups)
    kets[0] = to_previous_pool(bras[0])
    anchor = me.reshape(1, 1)
    for place, d in enumerate(arrivals):
        bras[d] = swapped_with(pieces[d], d)
        kets[d] = to_previous_pool(bras[d])
        if place == len(arrivals) - 1:
            break
        anchor = zero_like(anchor)
        if place == len(arrivals) - 2:
            before_last = anchor
        if place == 2:
            bra_info = jnp.stack(info) + anchor
    ket_info = to_previous_pool(bra_info)
    ket_of = pair_list(bra_info, ket_info + before_last, groups, slots, me)
    if (waves // groups) % 16:
        parts = multiply_plainly(bras, kets, ket_of, me, groups, scale)
    else:
        parts = multiply(bras, kets, ket_of, me, groups, scale)
    return reduce_to_owner(parts, groups)[None]


def arrival_order(groups):
    near = list(range(1, groups // 2))
    return [*near[:-1], groups // 2, near[-1], *range(groups // 2 + 1, groups)]


def solution(mesh):
    spec = P("pool", "ga")
    return jax.shard_map(
        local,
        mesh=mesh,
        in_specs=(P("pool", "ga", None, None, None), spec, spec, spec, spec),
        out_specs=P("pool", None, "ga", None),
        check_vma=False,
    )
```

```python
import jax
import jax.numpy as jnp
from jax import lax
from jax.experimental import pallas as pl
from jax.experimental.pallas import tpu as pltpu
from jax.sharding import PartitionSpec as P


def swapped_with(value, distance):
    count = lax.axis_size("ga")
    return lax.ppermute(value, "ga", [(i, i ^ distance) for i in range(count)])


def to_previous_pool(value):
    count = lax.axis_size("pool")
    return lax.ppermute(value, "pool", [(i, (i - 1) % count) for i in range(count)])


def pack(x, groups, me):
    slots, _, bands, waves = x.shape
    part = waves // groups
    if part % 16:
        cut = x.reshape(slots, 2, bands, groups, part).transpose(3, 1, 0, 4, 2)
        return [lax.dynamic_index_in_dim(cut, me ^ d, 0, False) for d in range(groups)]
    step = 4 if slots % 4 == 0 else 1

    def body(select_ref, x_ref, *refs):
        outs, held, sem = refs[:groups], refs[groups], refs[groups + 1]
        copies = [
            pltpu.make_async_copy(
                x_ref.at[pl.ds(i * step, step)], held.at[pl.ds(i * step, step)], sem.at[i]
            )
            for i in range(slots // step)
        ]
        for copy in copies:
            copy.start()
        for i, copy in enumerate(copies):
            copy.wait()
            for s in range(i * step, (i + 1) * step):
                for c in range(2):
                    turned = lax.dot_general(
                        select_ref[...],
                        held[s, c],
                        (((1,), (1,)), ((), ())),
                        preferred_element_type=jnp.float32,
                    ).astype(jnp.bfloat16)
                    for d in range(groups):
                        outs[d][c, s] = turned[d * part : (d + 1) * part]

    row = jnp.arange(waves, dtype=jnp.int32)
    source = ((row // part) ^ me) * part + row % part
    select = (source[:, None] == row[None, :]).astype(jnp.bfloat16)
    near = pl.BlockSpec(memory_space=pltpu.VMEM)
    return pl.pallas_call(
        body,
        in_specs=[near, pl.BlockSpec(memory_space=pltpu.HBM)],
        out_specs=[near] * groups,
        out_shape=[jax.ShapeDtypeStruct((2, slots, part, bands), jnp.bfloat16)] * groups,
        scratch_shapes=[
            pltpu.VMEM((slots, 2, bands, waves), jnp.bfloat16),
            pltpu.SemaphoreType.DMA((slots // step,)),
        ],
        compiler_params=pltpu.CompilerParams(vmem_limit_bytes=48 << 20),
        cost_estimate=pl.CostEstimate(
            flops=4 * slots * waves * waves * bands, bytes_accessed=x.size * 4, transcendentals=0
        ),
    )(select, x)


def passed_around(mine, groups):
    rows = [mine]
    for d in range(1, groups):
        rows.append(swapped_with(mine, d))
    return rows


def pair_list(bra_info, ket_info, groups, slots, me):
    counts = bra_info[:, 0]
    maps = ket_info[:, 1:].reshape(groups, 3, slots)
    device, slot, anchor = (maps[:, i].reshape(groups * slots) for i in range(3))
    number = jnp.arange(groups * slots, dtype=jnp.int32)
    here = ((number // slots) ^ me) * slots + number % slots
    lands = jnp.where(device >= 0, device * slots + slot, -1)
    live = (number % slots).reshape(groups, slots) < counts[:, None]
    agreeing = (anchor[:, None] == here[None, :]) & (lands[None, :] == here[:, None])
    agreeing &= live.reshape(-1)[:, None]
    return jnp.max(jnp.where(agreeing, number[None, :], -1), axis=1)


def multiply_plainly(bras, kets, ket_of, me, groups, scale):
    _, _, _, bands = bras[0].shape
    bra = jnp.concatenate(bras, axis=1)
    ket = jnp.concatenate(kets, axis=1)[:, jnp.maximum(ket_of, 0)]
    ket = jnp.where((ket_of >= 0)[None, :, None, None], ket, jnp.zeros_like(ket))

    def dot(a, b):
        return jnp.einsum("trm,trn->mn", bra[a], ket[b], preferred_element_type=jnp.float32)

    total = jnp.stack([dot(0, 0) + dot(1, 1), dot(0, 1) - dot(1, 0)]) * scale
    total = total.reshape(2, groups, bands // groups, bands)
    total = total[:, jnp.arange(groups, dtype=jnp.int32) ^ me]
    plan = halving_plan(groups)
    return [total[c][jnp.array(blocks)] for c in range(2) for blocks in plan[c][0]]


def multiply(bras, kets, ket_of, me, groups, scale):
    _, slots, part, bands = bras[0].shape
    rows = bands // groups
    depth = slots * part
    early = groups - 1
    near = pl.BlockSpec(memory_space=pltpu.VMEM)
    scalar = pl.BlockSpec(memory_space=pltpu.SMEM)

    def turned(chosen, d):
        first = chosen[0, d * slots : (d + 1) * slots].reshape(depth, bands).T
        second = chosen[1, d * slots : (d + 1) * slots].reshape(depth, bands).T
        upper = jnp.concatenate([first, second], axis=1)
        lower = jnp.concatenate([-second, first], axis=1)
        return jnp.concatenate([upper, lower], axis=0)

    def flat(ket_ref):
        return ket_ref[...].reshape(2 * depth, bands)

    def most(ket_of_ref, *refs):
        bra_refs, ket_refs = refs[:groups], refs[groups : groups + early]
        total_ref, last_ref, chosen = refs[groups + early :]
        chosen[...] = jnp.zeros_like(chosen)
        for d in range(groups):

            def put(s, _, d=d):
                row = ket_of_ref[d * slots + s]
                row = jnp.where(row >= 0, row, groups * slots)
                for c in range(2):
                    chosen[c, row] = bra_refs[d][c, s]
                return 0

            lax.fori_loop(0, slots, put, 0, unroll=8)
        for d in range(early):
            product = jnp.dot(turned(chosen, d), flat(ket_refs[d]), preferred_element_type=jnp.float32)
            if d == 0:
                total_ref[...] = product
            else:
                total_ref[...] += product
        last_ref[...] = turned(chosen, early)

    plan = halving_plan(groups)

    def rest(me_ref, total_ref, last_ref, ket_ref, *refs):
        outs, sums = refs[:-1], refs[-1]
        sums[...] = total_ref[...] + jnp.dot(
            last_ref[...], flat(ket_ref), preferred_element_type=jnp.float32
        )
        for c in range(2):
            for out, blocks in zip(outs[2 * c : 2 * c + 2], plan[c][0]):
                for place, d in enumerate(blocks):
                    start = c * bands + (me_ref[0] ^ d) * rows
                    out[place] = sums[pl.ds(pl.multiple_of(start, rows), rows)] * scale

    flops = 8 * depth * bands * bands
    total, last = pl.pallas_call(
        most,
        in_specs=[scalar] + [near] * (groups + early),
        out_specs=[near, near],
        out_shape=[
            jax.ShapeDtypeStruct((2 * bands, bands), jnp.float32),
            jax.ShapeDtypeStruct((2 * bands, 2 * depth), jnp.bfloat16),
        ],
        scratch_shapes=[pltpu.VMEM((2, groups * slots + 1, part, bands), jnp.bfloat16)],
        compiler_params=pltpu.CompilerParams(vmem_limit_bytes=32 << 20),
        cost_estimate=pl.CostEstimate(flops=early * flops, bytes_accessed=1 << 20, transcendentals=0),
    )(ket_of, *bras, *kets[:early])
    half = jax.ShapeDtypeStruct((groups // 2, rows, bands), jnp.float32)
    return pl.pallas_call(
        rest,
        in_specs=[scalar, near, near, near],
        out_specs=[near] * 4,
        out_shape=[half] * 4,
        scratch_shapes=[pltpu.VMEM((2 * bands, bands), jnp.float32)],
        compiler_params=pltpu.CompilerParams(vmem_limit_bytes=16 << 20),
        cost_estimate=pl.CostEstimate(flops=flops, bytes_accessed=1 << 20, transcendentals=0),
    )(me.reshape(1), total, last, kets[early])


def halving_plan(groups):
    bits = groups.bit_length() - 1
    plans = []
    for order in ([*range(bits)], [1, 0, *range(2, bits)]):
        blocks, steps = list(range(groups)), []
        for bit in order:
            kept = [i for i in blocks if not i >> bit & 1]
            steps.append(([i | 1 << bit for i in kept], kept))
            blocks = kept
        plans.append((steps[0], order, steps))
    return plans


def reduce_to_owner(parts, groups):
    plan = halving_plan(groups)
    gives, keeps = [parts[0], parts[2]], [parts[1], parts[3]]
    _, rows, bands = gives[0].shape
    steps = groups.bit_length() - 1
    near = pl.BlockSpec(memory_space=pltpu.VMEM)
    for step in range(steps):
        bits = [plan[c][1][step] for c in range(2)]
        if bits[0] == bits[1] and len(gives) == 1:
            got = [swapped_with(gives[0], 1 << bits[0])]
        else:
            got = [swapped_with(gives[c], 1 << bits[c]) for c in range(2)]
        if step == steps - 1:
            break
        joined = plan[0][1][step + 1] == plan[1][1][step + 1]
        count = groups >> (step + 2)

        def body(*refs, step=step, joined=joined, count=count, number=len(got)):
            held, come, outs = refs[:number], refs[number : 2 * number], refs[2 * number :]
            for c in range(2):
                steps_of = plan[c][2]
                now = steps_of[step][1]
                for kind in range(2):
                    for place, block in enumerate(steps_of[step + 1][kind]):
                        at = now.index(block)
                        source = (c, at) if number == 1 else (at,)
                        which = 0 if number == 1 else c
                        value = held[which][source] + come[which][source]
                        if joined:
                            outs[kind][c, place] = value
                        else:
                            outs[2 * c + kind][place] = value

        if joined:
            shapes = [jax.ShapeDtypeStruct((2, count, rows, bands), jnp.float32)] * 2
        else:
            shapes = [jax.ShapeDtypeStruct((count, rows, bands), jnp.float32)] * 4
        outs = pl.pallas_call(
            body,
            in_specs=[near] * (2 * len(got)),
            out_specs=[near] * len(shapes),
            out_shape=shapes,
            compiler_params=pltpu.CompilerParams(vmem_limit_bytes=8 << 20),
        )(*keeps, *got)
        gives, keeps = outs[0::2], outs[1::2]
    if len(keeps) == 1:
        return (keeps[0] + got[0])[:, 0]
    return jnp.stack([(keep + come)[0] for keep, come in zip(keeps, got)])


def zero_like(value):
    def body(_, out_ref):
        out_ref[0, 0] = 0

    scalar = pl.BlockSpec(memory_space=pltpu.SMEM)
    return pl.pallas_call(
        body,
        in_specs=[scalar],
        out_specs=scalar,
        out_shape=jax.ShapeDtypeStruct((1, 1), jnp.int32),
        compiler_params=pltpu.CompilerParams(vmem_limit_bytes=1 << 20),
    )(value)


def local(coefficients, stick_count, dest_device, dest_slot, source_stick):
    groups = lax.axis_size("ga")
    me = lax.axis_index("ga").astype(jnp.int32)
    _, slots, _, _, waves = coefficients.shape
    scale = (2 * groups * slots * waves) ** (-0.5)
    pieces = pack(coefficients[0], groups, me)
    mine = jnp.concatenate([stick_count, dest_device, dest_slot, source_stick], axis=1)[0]
    info = passed_around(mine, groups)
    bras, kets = [None] * groups, [None] * groups
    bras[0] = pieces[0]
    arrivals = range(1, groups)
    kets[0] = to_previous_pool(bras[0])
    anchor = me.reshape(1, 1)
    for place, d in enumerate(arrivals):
        bras[d] = swapped_with(pieces[d], d)
        kets[d] = to_previous_pool(bras[d])
        if place == len(arrivals) - 1:
            break
        anchor = zero_like(anchor)
        if place == len(arrivals) - 2:
            before_last = anchor
        if place == groups // 2 - 1:
            bra_info = jnp.stack(info) + anchor
    ket_info = to_previous_pool(bra_info)
    ket_of = pair_list(bra_info, ket_info + before_last, groups, slots, me)
    if (waves // groups) % 16:
        parts = multiply_plainly(bras, kets, ket_of, me, groups, scale)
    else:
        parts = multiply(bras, kets, ket_of, me, groups, scale)
    return reduce_to_owner(parts, groups)[None]


def solution(mesh):
    spec = P("pool", "ga")
    return jax.shard_map(
        local,
        mesh=mesh,
        in_specs=(P("pool", "ga", None, None, None), spec, spec, spec, spec),
        out_specs=P("pool", None, "ga", None),
        check_vma=False,
    )
```
